32 devices in a mesh: gx: 8 (over z, core), gy: 4 (over y, x).
Axes of the slice: x: 2, y: 2, z: 4, core: 2. Of those that a mesh axis runs over, the one named last changes fastest.
Arguments:
- density: float32 [512, 512, 512], P('gx', 'gy'), may hold values from -6 to 6
- radius_cells: int32 [2], replicated, may hold values from 1 to 32
Outputs:
- filtered: float32 [2, 512, 512, 512], P(None, 'gx', 'gy')
The draws below stay inside these ranges and needn't reach their ends.
All inputs are finite; a program needn't handle non-finite values.
Results may differ from the reference program's by a relative error of at most 0.0001.
Values sent between devices are 32-bit elements; how exact they have to be, the bound alone decides.
A program may use at most 192 MiB of HBM per device.

```python
import math
import jax
import jax.numpy as jnp

N = 512
RADII = 2


def block_scale(rng, dims, cuts, low, largest):
    gain = 1.0
    for dim, blocks in cuts:
        heights = jax.random.uniform(jax.random.fold_in(jax.random.fold_in(rng, 6), dim), (blocks,), jnp.float32, low / len(cuts), largest / len(cuts))
        gain = gain * jnp.repeat(jnp.exp(heights), dims[dim] // blocks).reshape((-1,) + (1,) * (len(dims) - 1 - dim))
    return gain


def normal_values(stream_key, shape, deviation, most, split=(), kind=jnp.bfloat16):
    level = block_scale(stream_key, shape, split, -0.22, 0.18) if split else 1.0
    values = jax.random.normal(stream_key, shape, jnp.float32) * deviation * level
    return jnp.minimum(jnp.maximum(values, -most), most).astype(kind)


def setup_inputs(seed: int = 0) -> dict:
    keys = jax.random.split(jax.random.key(seed), 3)
    density = normal_values(keys[0], (N, N, N), 1.0, 6.0, ((0, 8), (1, 4)), jnp.float32)
    radius_cells = jax.random.randint(keys[1], (RADII,), 1, 33).astype(jnp.int32)
    return {"density": density, "radius_cells": radius_cells}


def window(u_value):
    is_small = u_value < 0.2
    safe_u = jnp.where(is_small, 1.0, u_value)
    closed_form = 3.0 * (jnp.sin(safe_u) - safe_u * jnp.cos(safe_u)) / (safe_u * safe_u * safe_u)
    series = 1.0 - u_value * u_value / 10.0 + u_value ** 4 / 280.0
    return jnp.where(is_small, series, closed_form)

def reference(density, radius_cells):
    spectrum = jnp.fft.fftn(density)
    indices = jnp.arange(N, dtype=jnp.int32)
    signed = jnp.where(indices > N // 2, indices - N, indices).astype(jnp.float32)
    squares = signed * signed
    k_squared = squares[:, None, None] + squares[None, :, None] + squares[None, None, :]
    k_length = 2.0 * math.pi / N * jnp.sqrt(k_squared)
    results = []
    for radius_index in range(RADII):
        weights = window(k_length * radius_cells[radius_index].astype(jnp.float32))
        results.append(jnp.real(jnp.fft.ifftn(spectrum * weights)).astype(jnp.float32))
    return jnp.stack(results)
```

```python
import math

import jax
import jax.numpy as jnp
import numpy as np
from jax import lax
from jax.sharding import PartitionSpec as P

PREC = lax.Precision.HIGH


def window(k_squared, scale_squared):
    u_squared = k_squared * scale_squared
    u_value = jnp.sqrt(u_squared)
    is_small = u_value < 0.2
    safe = jnp.where(is_small, 1.0, u_value)
    turns = jnp.floor(safe * (1.0 / math.pi) + 0.5)
    rest = safe - turns * 3.140625
    rest = rest - turns * 9.67502593994140625e-4
    rest = rest - turns * 1.509957990978376432e-7
    s2 = rest * rest
    sin_v = rest * (1.0 + s2 * (-1.6666666666e-1 + s2 * (8.3333333e-3 + s2 * (
        -1.98412698e-4 + s2 * (2.75573192e-6 + s2 * -2.50521084e-8)))))
    cos_v = 1.0 + s2 * (-0.5 + s2 * (4.16666666e-2 + s2 * (-1.38888889e-3 + s2 * (
        2.48015873e-5 + s2 * (-2.75573192e-7 + s2 * 2.08767570e-9)))))
    half = turns * 0.5
    sign = jnp.where(half == jnp.floor(half), 3.0, -3.0)
    closed = sign * (sin_v - safe * cos_v) / (safe * safe * safe)
    series = 1.0 - u_squared / 10.0 + u_squared * u_squared / 280.0
    return jnp.where(is_small, series, closed)


def times_i(values, half):
    return jnp.concatenate([-values[..., half:], values[..., :half]], -1)


def doubled(values, half):
    return jnp.concatenate([values, times_i(values, half)], 0)


def squares(values, length):
    signed = jnp.where(values > length // 2, values - length, values).astype(jnp.float32)
    return signed * signed


def dot(spec, left, right):
    return jnp.einsum(spec, left, right, precision=PREC, preferred_element_type=jnp.float32)


def trig(rows, cols, length):
    angles = 2.0 * math.pi / length * (np.outer(rows, cols) % length)
    return np.cos(angles), np.sin(angles)


def y_order(length, parts):
    half = length // parts // 2
    base = np.arange(length // 2).reshape(parts, half)
    mirror = (length - base) % length
    mirror[0, 0] = length // 2
    return np.concatenate([base, mirror], 1).reshape(-1)


def per_device(density, radius_cells):
    rows_x, rows_y, length = density.shape
    count_gx = lax.axis_size("gx")
    count_gy = lax.axis_size("gy")
    mid = length // 2
    half = mid // count_gy
    lanes = 2 * half
    cols_y = length // count_gx
    f32 = jnp.float32
    cells = np.arange(length)
    order = y_order(length, count_gx)

    cos_z, sin_z = trig(cells, np.arange(mid), length)
    fwd_im = -sin_z
    fwd_im[:, 0] = np.where(cells % 2 == 0, 1.0, -1.0)
    fwd_z = np.stack([cos_z, fwd_im], 1).reshape(length, 2, count_gy, half)
    fwd_z = jnp.asarray(fwd_z.transpose(2, 0, 1, 3).reshape(count_gy, length, lanes), f32)
    gain = np.full((mid,), 2.0 / float(length) ** 3)
    gain[0] = 1.0 / float(length) ** 3
    inv_re = cos_z * gain
    inv_im = -sin_z * gain
    inv_im[:, 0] = np.where(cells % 2 == 0, 1.0, -1.0) * gain[0]
    inv_z = np.stack([inv_re, inv_im], 1).reshape(length, 2, count_gy, half)
    inv_z = jnp.asarray(inv_z.transpose(2, 1, 3, 0).reshape(length, length), f32)
    cos_y, sin_y = trig(order, cells, length)
    fwd_y = jnp.asarray(np.concatenate([cos_y, sin_y], 1), f32)
    fwd_y = fwd_y * jnp.where(jnp.arange(2 * length) < length, 1.0, -1.0)
    inv_y = jnp.asarray(np.concatenate([cos_y.T, sin_y.T], 1), f32)
    cos_x, sin_x = trig(cells, cells, length)
    inv_x = jnp.asarray(np.concatenate([cos_x, sin_x], 1), f32)
    fwd_x = inv_x * jnp.where(jnp.arange(2 * length) < length, 1.0, -1.0)

    values = dot("xyz,bzl->byxl", density, fwd_z)
    values = lax.all_to_all(values, "gy", split_axis=0, concat_axis=0, tiled=True)
    values = values.reshape(length, rows_x, lanes)
    values = dot("qy,yxl->qxl", fwd_y, doubled(values, half))
    values = values.reshape(count_gx, cols_y, rows_x, lanes).transpose(0, 2, 1, 3)
    values = lax.all_to_all(values, "gx", split_axis=0, concat_axis=0, tiled=True)
    values = values.reshape(length, cols_y, lanes)
    values = dot("kx,xql->kql", fwd_x, doubled(values, half))

    part_x = lax.axis_index("gx")
    part_y = lax.axis_index("gy")
    kx_sq = squares(jnp.arange(length, dtype=jnp.int32), length)
    local = jnp.arange(cols_y, dtype=jnp.int32)
    base = part_x * (cols_y // 2) + local % (cols_y // 2)
    ky = jnp.where(local < cols_y // 2, base, (length - base) % length)
    ky = jnp.where((part_x == 0) & (local == cols_y // 2), mid, ky)
    ky_sq = squares(ky, length)
    lane = jnp.arange(lanes, dtype=jnp.int32)
    kz_sq = squares(part_y * half + lane % half, length)
    plane_sq = kx_sq[:, None] + ky_sq[None, :]
    cube_sq = plane_sq[:, :, None] + kz_sq[None, None, :]

    own_re = values[:, :, 0]
    own_im = values[:, :, half]

    def mirror(plane):
        plane = jnp.roll(jnp.flip(plane, 0), 1, 0)
        swapped = jnp.roll(plane, cols_y // 2, 1)
        itself = (part_x == 0) & (local % (cols_y // 2) == 0)
        return jnp.where(itself[None, :], plane, swapped)

    far_re, far_im = mirror(own_re), mirror(own_im)
    first = part_y == 0
    outs = []
    for index in range(radius_cells.shape[0]):
        scale = 2.0 * math.pi / length * radius_cells[index].astype(f32)
        scale = scale * scale
        weight = window(cube_sq, scale)
        low = window(plane_sq, scale)
        high = window(plane_sq + float(mid) ** 2, scale)
        mean, diff = 0.5 * (low + high), 0.5 * (low - high)
        fix_re = own_re * mean + far_re * diff
        fix_im = own_im * mean - far_im * diff
        field = values * weight
        field = jnp.where(first & (lane == 0), fix_re[:, :, None], field)
        field = jnp.where(first & (lane == half), fix_im[:, :, None], field)
        field = dot("xk,kql->xql", inv_x, doubled(field, half))
        field = field.reshape(count_gx, rows_x, cols_y, lanes)
        outs.append(lax.all_to_all(field, "gx", split_axis=0, concat_axis=0, tiled=True))
    results = []
    for field in outs:
        field = field.transpose(0, 2, 1, 3).reshape(length, rows_x, lanes)
        field = dot("yq,qxl->yxl", inv_y, doubled(field, half))
        field = field.reshape(count_gy, rows_y, rows_x, lanes)
        field = lax.all_to_all(field, "gy", split_axis=0, concat_axis=0, tiled=True)
        field = dot("gyxl,glz->xyz", field, inv_z.reshape(count_gy, lanes, length))
        results.append(field)
    return jnp.stack(results)


def solution(mesh):
    return jax.shard_map(
        per_device,
        mesh=mesh,
        in_specs=(P("gx", "gy", None), P()),
        out_specs=P(None, "gx", "gy", None),
        check_vma=False,
    )
```
